32 devices in a mesh: seq: 8 (over z, y), grp: 4 (over x, core).
Axes of the slice: x: 2, y: 2, z: 4, core: 2. Of those that a mesh axis runs over, the one named last changes fastest.
Arguments:
- query_nope: bfloat16 [4, 2, 128, 128], P(None, None, 'seq'), may hold values from -12.859821 to 12.859821
- query_rope: bfloat16 [4, 2, 128, 64], P(None, None, 'seq'), may hold values from -150 to 150
- latent_cache: bfloat16 [4, 8192, 576], P(None, ('seq', 'grp')), may hold values from -5 to 5
- lengths: int32 [4], replicated, may hold values from 4096 to 8192
- key_weight: bfloat16 [128, 128, 512], P('seq'), may hold values from -0.5 to 0.5
- value_weight: bfloat16 [128, 512, 128], P('seq'), may hold values from -0.25 to 0.25
- output_weight: bfloat16 [16384, 7168], P('seq', 'grp'), may hold values from -0.0625 to 0.0625
Outputs:
- mixed: bfloat16 [4, 2, 7168], P(None, None, ('grp', 'seq'))
The draws below stay inside these ranges and needn't reach their ends.
All inputs are finite; a program needn't handle non-finite values.
Results may differ from the reference program's by a relative error of at most 0.0095.
Values may be sent and summed in bfloat16 or wider, within the bound.
No kernel may reach another device: no remote copies, remote signals or barrier semaphores. Data moves between devices by JAX's collectives and lax.ppermute only.
A program may use at most 64 MiB of HBM per device.

```python
import math
import jax
import jax.numpy as jnp
from jax import lax

H = 128
DL = 512
DR = 64
DN = 128
DV = 128
DM = 7168
B = 4
QT = 2
CTX_DEV = 256
SEQ = 8192
N_SEQ = 8
N_GRP = 4


echo_shrink = 0.008


def anchor_plan(key):
    subkeys = jax.random.split(jax.random.fold_in(key, 613), 8)
    sign_flip = jnp.where(jax.random.bernoulli(subkeys[0], 0.5, (B, DR)), 1.0, -1.0)
    anchor = 5.0 * sign_flip * jax.random.uniform(subkeys[1], (B, DR), jnp.float32, 0.8, 1.0)
    anchor_at = jax.random.randint(subkeys[2], (B,), 0, SEQ // 4 - 1)
    class_pick = jax.random.uniform(subkeys[3], (B, QT, H, 1), jnp.float32)
    strong_heads = class_pick < -1.0
    drawn_heads = jnp.logical_and(class_pick >= 0.125, class_pick < 0.375)
    drawn_target = jax.random.uniform(subkeys[4], (B, QT, H, 1), jnp.float32, 11.0, 15.0)
    strong_target = jax.random.uniform(subkeys[5], (B, QT, H, 1), jnp.float32, 150.0, 330.0)
    blend = jax.random.uniform(subkeys[6], (B, QT, H, 1), jnp.float32, 0.0, 1.5)
    crosswise = jax.random.normal(subkeys[7], (B, QT, H, DR), jnp.float32)
    return (anchor, anchor_at, strong_heads, drawn_heads, drawn_target, strong_target, blend, crosswise)


def draw_latent_cache(key, part):
    anchor, anchor_at, strong_heads, drawn_heads, drawn_target, strong_target, blend, crosswise = anchor_plan(key)
    subkeys = jax.random.split(jax.random.fold_in(key, 271), 3)
    latent = jnp.clip(jax.random.normal(subkeys[1], (B, SEQ, DL), jnp.float32), -5.0, 5.0)
    rotary = jnp.clip(jax.random.normal(subkeys[2], (B, SEQ, DR), jnp.float32), -5.0, 5.0)
    positions = jnp.arange(SEQ, dtype=jnp.int32)[None, :, None]
    anchor_rows = anchor[:, None, :]
    rotary = jnp.where(positions == anchor_at[:, None, None], anchor_rows, rotary)
    rotary = jnp.where(positions == (anchor_at + SEQ // 4)[:, None, None], anchor_rows * (1.0 - echo_shrink), rotary)
    return jnp.concatenate([latent, rotary], axis=-1).astype(jnp.bfloat16)


def draw_query_nope(key, part):
    anchor, anchor_at, strong_heads, drawn_heads, drawn_target, strong_target, blend, crosswise = anchor_plan(key)
    spread = 3.5 * math.sqrt(DN + DR) / math.sqrt(DL)
    nope_key = jax.random.fold_in(key, 419)
    drawn_draw = jnp.clip(jax.random.normal(nope_key, (B, QT, H, DN), jnp.float32), -6.0, 6.0)
    factor = jnp.where(strong_heads, 0.1, jnp.where(drawn_heads, 0.4, 1.0))
    return (spread * factor * drawn_draw).astype(jnp.bfloat16)


def draw_query_rope(key, part):
    anchor, anchor_at, strong_heads, drawn_heads, drawn_target, strong_target, blend, crosswise = anchor_plan(key)
    rope_key = jax.random.fold_in(key, 523)
    drawn_draw = jnp.clip(2.0 * jax.random.normal(rope_key, (B, QT, H, DR), jnp.float32), -12.0, 12.0)
    anchors = anchor[:, None, None, :]
    squared = jnp.sum(anchors * anchors, axis=-1, keepdims=True)
    parallel = jnp.sum(crosswise * anchors, axis=-1, keepdims=True) / squared
    across = crosswise - parallel * anchors
    across = across / jnp.sqrt(jnp.sum(across * across, axis=-1, keepdims=True) + 1e-06)
    direction = anchors + blend * jnp.sqrt(squared) * across
    root_width = math.sqrt(DN + DR)
    strong_query = strong_target * root_width / squared * direction
    drawn_query = drawn_target * root_width / squared * anchors
    queries = jnp.where(strong_heads, strong_query, jnp.where(drawn_heads, drawn_query, drawn_draw))
    return jnp.clip(queries, -150.0, 150.0).astype(jnp.bfloat16)


def plant(result, stream_key, smallest, high):
    place = [jax.random.randint(jax.random.fold_in(stream_key, axis), (), 0, length) for axis, length in enumerate(result.shape)]
    widest = result.shape.index(max(result.shape))
    next_to = place[:widest] + [(place[widest] + 1) % result.shape[widest]] + place[widest + 1:]
    return result.at[tuple(place)].set(smallest).at[tuple(next_to)].set(high)


def spiked(array, own_key, source, target, blocks, factor):
    owner, partner = [(jnp.arange(array.shape[axis_at]) // (array.shape[axis_at] // blocks)).reshape([-1 if axis == axis_at else 1 for axis in range(array.ndim)]) for axis_at in (source, target)]
    chosen = jax.random.permutation(own_key, blocks)[partner]
    strong = (owner == chosen) | (owner == (partner + blocks // 2) % blocks)
    return jnp.where(strong, factor * array, array)


def levels(own_key, extent, pieces, low, largest):
    def one(dim, shards_of):
        steps = jax.random.uniform(jax.random.fold_in(jax.random.fold_in(own_key, 6), dim), (shards_of,), jnp.float32, low / len(pieces), largest / len(pieces))
        return jnp.repeat(jnp.exp(steps), extent[dim] // shards_of).reshape((-1,) + (1,) * (len(extent) - dim - 1))

    level = one(*pieces[0])
    for cut in pieces[1:]:
        level = level * one(*cut)
    return level


def scatter_about(own_key, extent, deviation, reach, cuts=(), held_as=jnp.bfloat16):
    values = deviation * jax.random.normal(own_key, extent, jnp.float32)
    if cuts:
        values = values * levels(own_key, extent, cuts, -0.22, 0.18)
    return jnp.clip(values, -reach, reach).astype(held_as)


def gaussian_with(own_key, extent, scale, reach, cuts, heavy, held_as=jnp.bfloat16):
    array = scale * jax.random.normal(own_key, extent, jnp.float32)
    if cuts:
        array = array * levels(own_key, extent, cuts, -0.22, 0.18)
    return jnp.clip(spiked(array, jax.random.fold_in(own_key, 3), *heavy), -reach, reach).astype(held_as)


def setup_inputs(seed: int = 0) -> dict:
    seeds = jax.random.split(jax.random.key(seed), 8)
    return {
        "query_nope": draw_query_nope(jax.random.fold_in(seeds[7], 71), 0),
        "query_rope": draw_query_rope(jax.random.fold_in(seeds[7], 71), 0),
        "latent_cache": draw_latent_cache(jax.random.fold_in(seeds[7], 71), 0),
        "lengths": plant(jax.random.randint(seeds[3], (B,), SEQ // 2, SEQ + 1), jax.random.fold_in(seeds[3], 1), SEQ // 2, SEQ).astype(jnp.int32),
        "key_weight": scatter_about(seeds[4], (H, DN, DL), DN ** -0.5, 0.5, ((0, 8),)),
        "value_weight": scatter_about(seeds[5], (H, DL, DV), DL ** -0.5, 0.25, ((0, 8),)),
        "output_weight": gaussian_with(seeds[6], (H * DV, DM), (H * DV) ** -0.5, 0.0625, ((0, 8), (1, 4)), (0, 1, 8, 2.0)),
    }


NEGATIVE = -1e30


def shard_partial(queries, cache_block, limits, offset):
    raw_score = jnp.einsum("bqhd,bpd->bqhp", queries.astype(jnp.float32), cache_block.astype(jnp.float32)) * ((DN + DR) ** -0.5)
    places = offset + jnp.arange(CTX_DEV, dtype=jnp.int32)
    visible = places[None, None, :] < limits[:, :, None]
    scores = jnp.where(visible[:, :, None, :], raw_score, NEGATIVE)
    maxima = jnp.max(scores, axis=-1)
    powers = jnp.exp(scores - maxima[..., None])
    totals = jnp.sum(powers, axis=-1)
    weights = lax.optimization_barrier(powers.astype(jnp.bfloat16))
    summed = jnp.einsum("bqhp,bpd->bqhd", weights.astype(jnp.float32), cache_block[:, :, :DL].astype(jnp.float32))
    partials = (summed / totals[..., None]).astype(jnp.bfloat16)
    return maxima, totals, partials


def reference(query_nope, query_rope, latent_cache, lengths, key_weight, value_weight, output_weight):
    absorbed = jnp.einsum("bqhn,hnd->bqhd", query_nope.astype(jnp.float32), key_weight.astype(jnp.float32))
    absorbed = absorbed.astype(jnp.bfloat16)
    queries = jnp.concatenate([absorbed, query_rope], axis=-1)
    limits = lengths[:, None] - QT + 1 + jnp.arange(QT, dtype=jnp.int32)[None, :]

    def visit_shard(carried, shard_index):
        highest, summed, numerator = carried
        offset = (shard_index * CTX_DEV).astype(jnp.int32)
        cache_block = lax.dynamic_slice_in_dim(latent_cache, offset, CTX_DEV, 1)
        maxima, totals, partials = shard_partial(queries, cache_block, limits, offset)
        partials = lax.optimization_barrier(partials)
        raised = jnp.maximum(highest, maxima)
        rescale = jnp.exp(highest - raised)
        shares = totals * jnp.exp(maxima - raised)
        numerator = numerator * rescale[..., None] + shares[..., None] * partials.astype(jnp.float32)
        return (raised, summed * rescale + shares, numerator), None

    start_state = (jnp.full((B, QT, H), NEGATIVE, jnp.float32), jnp.zeros((B, QT, H), jnp.float32), jnp.zeros((B, QT, H, DL), jnp.float32))
    final_state, unused = lax.scan(visit_shard, start_state, jnp.arange(N_SEQ * N_GRP, dtype=jnp.int32))
    latent_out = lax.optimization_barrier((final_state[2] / final_state[1][..., None]).astype(jnp.bfloat16))
    values = jnp.einsum("bqhd,hde->bqhe", latent_out.astype(jnp.float32), value_weight.astype(jnp.float32)).astype(jnp.bfloat16)
    projected = jnp.dot(values.reshape(B * QT, H * DV), output_weight, preferred_element_type=jnp.float32)
    return projected.reshape(B, QT, DM).astype(jnp.bfloat16)
```

```python
import functools

import jax
import jax.numpy as jnp
from jax import lax
from jax.experimental import pallas as pl
from jax.experimental.pallas import tpu as pltpu
from jax.sharding import PartitionSpec as P

NEGATIVE = -1e30
LANES = 128


def split3(x):
    high = x.astype(jnp.bfloat16).astype(jnp.float32)
    rest = x - high
    middle = rest.astype(jnp.bfloat16).astype(jnp.float32)
    return high, middle, rest - middle


def attention_kernel(
    factor, latent, heads, offsets, limits, query, *refs
):
    caches, out = refs[:-1], refs[-1]
    rows = query.shape[0]
    width = caches[0].shape[1]
    drafts = limits.shape[0]
    token = (lax.broadcasted_iota(jnp.int32, (rows, 1), 0) // heads) % drafts
    limit = jnp.full((rows, 1), limits[0], jnp.int32)
    for t in range(1, drafts):
        limit = jnp.where(token == t, limits[t], limit)
    queries = query[...]
    scores = []
    for j, cache in enumerate(caches):
        raw = jnp.dot(queries, cache[...], preferred_element_type=jnp.float32) * factor
        places = offsets[j] + lax.broadcasted_iota(jnp.int32, (rows, width), 1)
        scores.append(jnp.where(places < limit, raw, NEGATIVE))
    top = functools.reduce(jnp.maximum, scores).max(axis=-1, keepdims=True)
    total = jnp.zeros((rows, 1), jnp.float32)
    summed = jnp.zeros((rows, latent), jnp.float32)
    for j, cache in enumerate(caches):
        expo = jnp.exp(scores[j] - top)
        total = total + jnp.sum(expo, axis=-1, keepdims=True)
        summed = summed + lax.dot_general(
            expo.astype(jnp.bfloat16),
            cache[:latent, :],
            (((1,), (1,)), ((), ())),
            preferred_element_type=jnp.float32,
        )
    out[:, :latent] = (summed / total).astype(jnp.bfloat16)
    lane = lax.broadcasted_iota(jnp.int32, (rows, LANES), 1)
    packed = jnp.zeros((rows, LANES), jnp.float32)
    for i, piece in enumerate(split3(top) + split3(total)):
        packed = jnp.where(lane == i, piece, packed)
    out[:, latent:] = packed.astype(jnp.bfloat16)


def merge_kernel(latent, received, out):
    block = received[...].astype(jnp.float32)
    stats = block[:, :, latent:]
    top = (stats[:, :, 0:1] + stats[:, :, 1:2]) + stats[:, :, 2:3]
    total = (stats[:, :, 3:4] + stats[:, :, 4:5]) + stats[:, :, 5:6]
    peak = jnp.max(top, axis=0, keepdims=True)
    share = total * jnp.exp(top - peak)
    numerator = jnp.sum(share * block[:, :, :latent], axis=0)
    out[...] = (numerator / jnp.sum(share, axis=0)).astype(jnp.bfloat16)


def whole(count):
    return [pl.BlockSpec(memory_space=pltpu.VMEM)] * count


def shards(query_nope, query_rope, latent_cache, lengths, key_weight, value_weight, output_weight):
    n_seq, n_grp = lax.axis_size("seq"), lax.axis_size("grp")
    seq, grp = lax.axis_index("seq"), lax.axis_index("grp")
    requests, drafts, heads, nope = query_nope.shape
    latent = key_weight.shape[2]
    positions, width = latent_cache.shape[1:]
    factor = float(nope + query_rope.shape[3]) ** (-0.5)
    assert requests == n_grp

    by_width = jnp.swapaxes(latent_cache, 1, 2)

    def request(array, index):
        return lax.dynamic_index_in_dim(array, index, 0, False)

    def partner(k):
        if n_grp & (n_grp - 1) == 0:
            return lambda i: i ^ k
        return lambda i: (k - i) % n_grp

    steps = range(n_grp)
    caches, holders = [], []
    for k in steps:
        other = partner(k)
        piece = request(by_width, other(grp))
        if k or other(1) != 1:
            piece = lax.ppermute(piece, "grp", [(i, other(i)) for i in range(n_grp)])
        caches.append(piece)
        holders.append(other(grp))
    offsets = jnp.stack([(seq * n_grp + holder) * positions for holder in holders])
    limits = request(lengths, grp) - drafts + 1 + jnp.arange(drafts, dtype=jnp.int32)

    absorbed = jnp.einsum(
        "qhn,hnd->qhd", request(query_nope, grp), key_weight, preferred_element_type=jnp.float32
    ).astype(jnp.bfloat16)
    own = jnp.concatenate([absorbed, request(query_rope, grp)], axis=-1)
    own = own.reshape(1, drafts * heads, width)
    queries = lax.all_to_all(
        jnp.broadcast_to(own, (n_seq,) + own.shape[1:]), "seq", 0, 0, tiled=True
    ).reshape(n_seq * drafts * heads, width)

    rows = n_seq * drafts * heads
    partial = pl.pallas_call(
        functools.partial(attention_kernel, factor, latent, heads),
        out_shape=jax.ShapeDtypeStruct((rows, latent + LANES), jnp.bfloat16),
        in_specs=[pl.BlockSpec(memory_space=pltpu.SMEM)] * 2 + whole(1 + n_grp),
        out_specs=pl.BlockSpec(memory_space=pltpu.VMEM),
        compiler_params=pltpu.CompilerParams(vmem_limit_bytes=12 << 20),
        name="attention",
    )(offsets, limits, queries, *caches)

    received = lax.all_to_all(
        partial.reshape(n_seq, drafts * heads, latent + LANES), "seq", 0, 0, tiled=True
    )
    latent_out = pl.pallas_call(
        functools.partial(merge_kernel, latent),
        out_shape=jax.ShapeDtypeStruct((drafts * heads, latent), jnp.bfloat16),
        in_specs=whole(1),
        out_specs=pl.BlockSpec(memory_space=pltpu.VMEM),
        compiler_params=pltpu.CompilerParams(vmem_limit_bytes=4 << 20),
        name="merge",
    )(received)

    values = jnp.einsum(
        "qhd,hde->qhe",
        latent_out.reshape(drafts, heads, latent),
        value_weight,
        preferred_element_type=jnp.float32,
    ).astype(jnp.bfloat16)
    values = lax.all_gather(values.reshape(drafts, -1), "grp", axis=0, tiled=True)
    terms = jnp.dot(values, output_weight, preferred_element_type=jnp.float32)
    tokens, columns = terms.shape
    terms = terms.reshape(tokens, n_seq, columns // n_seq).swapaxes(0, 1)
    terms = lax.all_to_all(terms, "seq", 0, 0, tiled=True)
    mixed = jnp.sum(terms, axis=0).astype(jnp.bfloat16)
    return mixed.reshape(requests, drafts, columns // n_seq)


def solution(mesh):
    in_specs = (
        P(None, None, "seq", None),
        P(None, None, "seq", None),
        P(None, ("seq", "grp"), None),
        P(),
        P("seq", None, None),
        P("seq", None, None),
        P("seq", "grp"),
    )
    out_specs = P(None, None, ("grp", "seq"))
    return jax.shard_map(shards, mesh=mesh, in_specs=in_specs, out_specs=out_specs, check_vma=False)
```

```python
import functools

import jax
import jax.numpy as jnp
from jax import lax
from jax.experimental import pallas as pl
from jax.experimental.pallas import tpu as pltpu
from jax.sharding import PartitionSpec as P


NEGATIVE = -1e30
LANES = 128


def split3(x):
    high = x.astype(jnp.bfloat16).astype(jnp.float32)
    rest = x - high
    middle = rest.astype(jnp.bfloat16).astype(jnp.float32)
    return high, middle, rest - middle


def attention_kernel(factor, latent, heads, drafts, partners, lengths, query, *refs):
    caches, out = refs[:-1], refs[-1]
    rows = query.shape[0]
    width = caches[0].shape[1]
    seq, grp = lax.axis_index("seq"), lax.axis_index("grp")
    token = (lax.broadcasted_iota(jnp.int32, (rows, 1), 0) // heads) % drafts
    limit = lengths[grp] - drafts + 1 + token
    queries = query[...]
    scores = []
    for j, cache in enumerate(caches):
        raw = jnp.dot(queries, cache[...], preferred_element_type=jnp.float32) * factor
        offset = (seq * len(caches) + partners[j](grp)) * width
        places = offset + lax.broadcasted_iota(jnp.int32, (rows, width), 1)
        scores.append(jnp.where(places < limit, raw, NEGATIVE))
    top = functools.reduce(jnp.maximum, scores).max(axis=-1, keepdims=True)
    total = jnp.zeros((rows, 1), jnp.float32)
    summed = jnp.zeros((rows, latent), jnp.float32)
    for j, cache in enumerate(caches):
        expo = jnp.exp(scores[j] - top)
        total = total + jnp.sum(expo, axis=-1, keepdims=True)
        summed = summed + lax.dot_general(
            expo.astype(jnp.bfloat16),
            cache[:latent, :],
            (((1,), (1,)), ((), ())),
            preferred_element_type=jnp.float32,
        )
    out[:, :latent] = (summed / total).astype(jnp.bfloat16)
    lane = lax.broadcasted_iota(jnp.int32, (rows, LANES), 1)
    packed = jnp.zeros((rows, LANES), jnp.float32)
    for i, piece in enumerate(split3(top) + split3(total)):
        packed = jnp.where(lane == i, piece, packed)
    out[:, latent:] = packed.astype(jnp.bfloat16)


def stacked(array, heads):
    rows = array.shape[0]
    head = lax.broadcasted_iota(jnp.int32, (rows, 1), 0) % heads
    zero = jnp.zeros_like(array)
    return jnp.concatenate([jnp.where(head == h, array, zero) for h in range(heads)], axis=-1)


def pick_kernel(partners, cache, *refs):
    pieces, sems = refs[:-1], refs[-1]
    grp = lax.axis_index("grp")
    copies = [
        pltpu.make_async_copy(cache.at[partners[i](grp)], piece, sems.at[i])
        for i, piece in enumerate(pieces)
    ]
    for copy in copies:
        copy.start()
    for copy in copies:
        copy.wait()


def absorb_kernel(nope, rope, weight, queries, nope_block, rope_block, weights, sems):
    grp = lax.axis_index("grp")
    copies = [
        pltpu.make_async_copy(weight, weights, sems.at[0]),
        pltpu.make_async_copy(nope.at[grp], nope_block, sems.at[1]),
        pltpu.make_async_copy(rope.at[grp], rope_block, sems.at[2]),
    ]
    for copy in copies:
        copy.start()
    for copy in copies[::-1]:
        copy.wait()
    heads, depth, latent = weights.shape
    absorbed = jnp.dot(
        stacked(nope_block[...], heads),
        weights[...].reshape(heads * depth, latent),
        preferred_element_type=jnp.float32,
    ).astype(jnp.bfloat16)
    tail = rope_block[...]
    for i in range(queries.shape[0]):
        queries[i, :, :latent] = absorbed
        queries[i, :, latent:] = tail


def merge_kernel(latent, received, weight, out):
    block = received[...].astype(jnp.float32)
    stats = block[:, :, latent:]
    top = (stats[:, :, 0:1] + stats[:, :, 1:2]) + stats[:, :, 2:3]
    total = (stats[:, :, 3:4] + stats[:, :, 4:5]) + stats[:, :, 5:6]
    peak = jnp.max(top, axis=0, keepdims=True)
    share = total * jnp.exp(top - peak)
    numerator = jnp.sum(share * block[:, :, :latent], axis=0)
    merged = (numerator / jnp.sum(share, axis=0)).astype(jnp.bfloat16)
    heads, depth, width = weight.shape
    weights = weight[...].reshape(heads * depth, width)
    values = jnp.dot(stacked(merged, heads), weights, preferred_element_type=jnp.float32)
    out[...] = values.astype(jnp.bfloat16)


def project_kernel(values, weight, out, wide):
    tokens = out.shape[1]
    heads = values.shape[0] // tokens
    wide[...] = values[...].astype(jnp.float32)
    left = jnp.concatenate(
        [wide[pl.ds(h, tokens, stride=heads), :] for h in range(heads)], axis=-1
    ).astype(jnp.bfloat16)
    terms = jnp.dot(left, weight[...], preferred_element_type=jnp.float32)
    width = out.shape[2]
    for i in range(out.shape[0]):
        out[i] = terms[:, i * width : (i + 1) * width]


def whole(count):
    return [pl.BlockSpec(memory_space=pltpu.VMEM)] * count


def in_hbm(array):
    return pltpu.with_memory_space_constraint(array, pltpu.HBM)


def kernel_params(mebibytes):
    return pltpu.CompilerParams(vmem_limit_bytes=mebibytes << 20)


def shards(query_nope, query_rope, latent_cache, lengths, key_weight, value_weight, output_weight):
    n_seq, n_grp = lax.axis_size("seq"), lax.axis_size("grp")
    requests, drafts, heads, nope = query_nope.shape
    rope = query_rope.shape[3]
    latent = key_weight.shape[2]
    positions, width = latent_cache.shape[1:]
    factor = float(nope + rope) ** (-0.5)
    rows = drafts * heads
    assert requests == n_grp

    def partner(k):
        if n_grp & (n_grp - 1) == 0:
            return lambda i: i ^ k
        return lambda i: (k - i) % n_grp

    partners = [partner(k) for k in range(n_grp)]
    by_width = jnp.swapaxes(latent_cache, 1, 2)
    smem = pl.BlockSpec(memory_space=pltpu.SMEM)
    hbm = pl.BlockSpec(memory_space=pltpu.HBM)
    routes = [[(i, other(i)) for i in range(n_grp)] for other in partners]
    kept = [k for k in range(n_grp) if all(i == j for i, j in routes[k])]
    pieces = pl.pallas_call(
        functools.partial(pick_kernel, partners),
        out_shape=[jax.ShapeDtypeStruct((width, positions), jnp.bfloat16)] * n_grp,
        in_specs=[hbm],
        out_specs=whole(n_grp),
        scratch_shapes=[pltpu.SemaphoreType.DMA((n_grp,))],
        compiler_params=kernel_params(4),
        name="pick",
    )(in_hbm(by_width))
    caches = []
    for k, piece in enumerate(pieces):
        caches.append(piece if k in kept else lax.ppermute(piece, "grp", routes[k]))
    queries = pl.pallas_call(
        absorb_kernel,
        out_shape=jax.ShapeDtypeStruct((n_seq, rows, width), jnp.bfloat16),
        in_specs=[hbm] * 3,
        out_specs=whole(1)[0],
        scratch_shapes=[
            pltpu.VMEM((rows, nope), jnp.bfloat16),
            pltpu.VMEM((rows, rope), jnp.bfloat16),
            pltpu.VMEM(key_weight.shape, jnp.bfloat16),
            pltpu.SemaphoreType.DMA((3,)),
        ],
        compiler_params=kernel_params(8),
        name="absorb",
    )(
        in_hbm(query_nope.reshape(requests, rows, nope)),
        in_hbm(query_rope.reshape(requests, rows, rope)),
        in_hbm(key_weight),
    )
    queries = lax.all_to_all(queries, "seq", 0, 0, tiled=True)

    partial = pl.pallas_call(
        functools.partial(attention_kernel, factor, latent, heads, drafts, partners),
        out_shape=jax.ShapeDtypeStruct((n_seq * rows, latent + LANES), jnp.bfloat16),
        in_specs=[smem] + whole(1 + n_grp),
        out_specs=whole(1)[0],
        compiler_params=kernel_params(12),
        cost_estimate=pl.CostEstimate(flops=6 * 10**9, transcendentals=0, bytes_accessed=3 << 20),
        name="attention",
    )(lengths, queries.reshape(n_seq * rows, width), *caches)

    received = lax.all_to_all(partial.reshape(n_seq, rows, latent + LANES), "seq", 0, 0, tiled=True)
    values = pl.pallas_call(
        functools.partial(merge_kernel, latent),
        out_shape=jax.ShapeDtypeStruct((rows, value_weight.shape[2]), jnp.bfloat16),
        in_specs=whole(2),
        out_specs=whole(1)[0],
        compiler_params=kernel_params(8),
        name="merge",
    )(received, value_weight)
    values = lax.all_gather(values, "grp", axis=0, tiled=True)

    tokens = requests * drafts
    columns = output_weight.shape[1] // n_seq
    terms = pl.pallas_call(
        project_kernel,
        out_shape=jax.ShapeDtypeStruct((n_seq, tokens, columns), jnp.float32),
        in_specs=whole(2),
        out_specs=whole(1)[0],
        scratch_shapes=[pltpu.VMEM(values.shape, jnp.float32)],
        compiler_params=kernel_params(12),
        name="project",
    )(values, output_weight)
    terms = lax.all_to_all(terms, "seq", 0, 0, tiled=True)
    mixed = jnp.sum(terms, axis=0).astype(jnp.bfloat16)
    return mixed.reshape(requests, drafts, columns)


def solution(mesh):
    in_specs = (
        P(None, None, "seq", None),
        P(None, None, "seq", None),
        P(None, ("seq", "grp"), None),
        P(),
        P("seq", None, None),
        P("seq", None, None),
        P("seq", "grp"),
    )
    out_specs = P(None, None, ("grp", "seq"))
    return jax.shard_map(shards, mesh=mesh, in_specs=in_specs, out_specs=out_specs, check_vma=False)
```

```python
import functools

import jax
import jax.numpy as jnp
from jax import lax
from jax.experimental import pallas as pl
from jax.experimental.pallas import tpu as pltpu
from jax.sharding import PartitionSpec as P


NEGATIVE = -1e30
LANES = 128
STATS = 8


def split3(x):
    high = x.astype(jnp.bfloat16).astype(jnp.float32)
    rest = x - high
    middle = rest.astype(jnp.bfloat16).astype(jnp.float32)
    return high, middle, rest - middle


def chunks(width):
    return range(width // LANES)


def packs(n_seq, drafts, heads, latent, rope):
    rows = drafts * heads
    return (
        heads % 16 == 0
        and latent % LANES == 0
        and drafts * rope == LANES
        and LANES % rows == 0
        and n_seq * rows % LANES == 0
    )


def unpack_queries(query, latent, heads, drafts):
    n_seq, _, lanes = query.shape
    rows = drafts * heads
    parts = [query[:, c * rows : (c + 1) * rows, :] for c in chunks(latent)]
    tail = query[:, len(parts) * rows :, :]
    owner = lax.broadcasted_iota(jnp.int32, tail.shape, 2) // (lanes // drafts)
    zero = jnp.zeros_like(tail)
    parts.append(
        jnp.concatenate([jnp.where(owner == t, tail, zero) for t in range(drafts)], axis=1)
    )
    return jnp.concatenate([part.reshape(n_seq * rows, lanes) for part in parts], axis=-1)


def attention_kernel(factor, latent, heads, drafts, partners, packed, lengths, query, *refs):
    caches, out = refs[:-1], refs[-1]
    rows = query.shape[0] * drafts * heads if packed else query.shape[0]
    width = caches[0].shape[1]
    seq, grp = lax.axis_index("seq"), lax.axis_index("grp")
    token = (lax.broadcasted_iota(jnp.int32, (rows, 1), 0) // heads) % drafts
    limit = lengths[grp] - drafts + 1 + token
    queries = unpack_queries(query, latent, heads, drafts) if packed else query[...]
    scores = []
    for j, cache in enumerate(caches):
        keys = cache[...]
        if packed:
            keys = jnp.concatenate([keys] + [cache[latent:, :]] * (drafts - 1), axis=0)
        raw = jnp.dot(queries, keys, preferred_element_type=jnp.float32) * factor
        offset = (seq * len(caches) + partners[j](grp)) * width
        places = offset + lax.broadcasted_iota(jnp.int32, (rows, width), 1)
        scores.append(jnp.where(places < limit, raw, NEGATIVE))
    top = functools.reduce(jnp.maximum, scores).max(axis=-1, keepdims=True)
    total = jnp.zeros((rows, 1), jnp.float32)
    summed = jnp.zeros((rows, latent), jnp.float32)
    for j, cache in enumerate(caches):
        expo = jnp.exp(scores[j] - top)
        total = total + jnp.sum(expo, axis=-1, keepdims=True)
        summed = summed + lax.dot_general(
            expo.astype(jnp.bfloat16),
            cache[:latent, :],
            (((1,), (1,)), ((), ())),
            preferred_element_type=jnp.float32,
        )
    result = (summed / total).astype(jnp.bfloat16)
    lane = lax.broadcasted_iota(jnp.int32, (rows, LANES), 1)
    stats = jnp.zeros((rows, LANES), jnp.float32)
    for i, piece in enumerate(split3(top) + split3(total)):
        stats = jnp.where(lane == i, piece, stats)
    if not packed:
        out[:, :latent] = result
        out[:, latent:] = stats.astype(jnp.bfloat16)
        return
    block = drafts * heads
    by_stat = stats.T[:STATS].astype(jnp.bfloat16)
    for i in range(rows // block):
        for c in chunks(latent):
            lanes = slice(c * LANES, (c + 1) * LANES)
            out[i, c * block : (c + 1) * block, :] = result[i * block : (i + 1) * block, lanes]
        start = i * block // LANES * LANES
        out[i, len(chunks(latent)) * block :, :] = by_stat[:, start : start + LANES]


def stacked(array, heads):
    rows = array.shape[0]
    head = lax.broadcasted_iota(jnp.int32, (rows, 1), 0) % heads
    zero = jnp.zeros_like(array)
    return jnp.concatenate([jnp.where(head == h, array, zero) for h in range(heads)], axis=-1)


def pick_kernel(partners, cache, *refs):
    pieces, sems = refs[:-1], refs[-1]
    grp = lax.axis_index("grp")
    copies = [
        pltpu.make_async_copy(cache.at[partners[i](grp)], piece, sems.at[i])
        for i, piece in enumerate(pieces)
    ]
    for copy in copies:
        copy.start()
    for copy in copies:
        copy.wait()


def absorb_kernel(drafts, packed, nope, rope, weight, queries):
    grp = lax.axis_index("grp")
    heads, depth, latent = weight.shape
    absorbed = jnp.dot(
        stacked(nope[grp], heads),
        weight[...].reshape(heads * depth, latent),
        preferred_element_type=jnp.float32,
    ).astype(jnp.bfloat16)
    tail = rope[grp]
    if not packed:
        for i in range(queries.shape[0]):
            queries[i, :, :latent] = absorbed
            queries[i, :, latent:] = tail
        return
    parts = [absorbed[:, c * LANES : (c + 1) * LANES] for c in chunks(latent)]
    parts.append(
        jnp.concatenate([tail[t * heads : (t + 1) * heads] for t in range(drafts)], axis=-1)
    )
    block = jnp.concatenate(parts, axis=0)
    for i in range(queries.shape[0]):
        queries[i] = block


def merge_kernel(latent, packed, received, weight, out, *scratch):
    heads, depth, width = weight.shape
    rows = out.shape[0]
    sources = received.shape[0]
    if packed:
        turned = scratch[0]
        first = len(chunks(latent)) * rows
        stats = received[:, first:, :].astype(jnp.float32).reshape(sources * STATS, LANES)
        turned[...] = stats.T
        start = lax.axis_index("seq") * rows % LANES
        own = turned[pl.ds(pl.multiple_of(start, rows), rows), :]
        columns = [[own[:, j * STATS + i : j * STATS + i + 1] for i in range(6)] for j in range(sources)]
        parts = [
            [received[j, c * rows : (c + 1) * rows, :] for j in range(sources)]
            for c in chunks(latent)
        ]
    else:
        block = received[...]
        stats = block[:, :, latent:].astype(jnp.float32)
        columns = [[stats[j, :, i : i + 1] for i in range(6)] for j in range(sources)]
        parts = [[block[j, :, :latent] for j in range(sources)]]
    tops = [(column[0] + column[1]) + column[2] for column in columns]
    peak = functools.reduce(jnp.maximum, tops)
    shares = [
        ((column[3] + column[4]) + column[5]) * jnp.exp(top - peak)
        for column, top in zip(columns, tops)
    ]
    summed = functools.reduce(jnp.add, shares)
    merged = jnp.concatenate(
        [
            functools.reduce(
                jnp.add, [share * piece.astype(jnp.float32) for share, piece in zip(shares, part)]
            )
            / summed
            for part in parts
        ],
        axis=-1,
    ).astype(jnp.bfloat16)
    values = jnp.dot(
        stacked(merged, heads),
        weight[...].reshape(heads * depth, width),
        preferred_element_type=jnp.float32,
    )
    out[...] = values.astype(jnp.bfloat16)


def project_kernel(values, weight, out, wide):
    tokens = out.shape[1]
    heads = values.shape[0] // tokens
    wide[...] = values[...].astype(jnp.float32)
    left = jnp.concatenate(
        [wide[pl.ds(h, tokens, stride=heads), :] for h in range(heads)], axis=-1
    ).astype(jnp.bfloat16)
    terms = jnp.dot(left, weight[...], preferred_element_type=jnp.float32)
    width = out.shape[2]
    for i in range(out.shape[0]):
        out[i] = terms[:, i * width : (i + 1) * width].astype(out.dtype)


def whole(count):
    return [pl.BlockSpec(memory_space=pltpu.VMEM)] * count


def in_hbm(array):
    return pltpu.with_memory_space_constraint(array, pltpu.HBM)


def kernel_params(mebibytes):
    return pltpu.CompilerParams(vmem_limit_bytes=mebibytes << 20)


def shards(query_nope, query_rope, latent_cache, lengths, key_weight, value_weight, output_weight):
    n_seq, n_grp = lax.axis_size("seq"), lax.axis_size("grp")
    requests, drafts, heads, nope = query_nope.shape
    rope = query_rope.shape[3]
    latent = key_weight.shape[2]
    positions, width = latent_cache.shape[1:]
    factor = float(nope + rope) ** (-0.5)
    rows = drafts * heads
    assert requests == n_grp
    packed = packs(n_seq, drafts, heads, latent, rope)
    asked = (rows * len(chunks(latent)) + heads, LANES) if packed else (rows, width)
    given = (rows * len(chunks(latent)) + STATS, LANES) if packed else (rows, latent + LANES)

    def partner(k):
        if n_grp & (n_grp - 1) == 0:
            return lambda i: i ^ k
        return lambda i: (k - i) % n_grp

    partners = [partner(k) for k in range(n_grp)]
    by_width = jnp.swapaxes(latent_cache, 1, 2)
    smem = pl.BlockSpec(memory_space=pltpu.SMEM)
    hbm = pl.BlockSpec(memory_space=pltpu.HBM)
    routes = [[(i, other(i)) for i in range(n_grp)] for other in partners]
    kept = [k for k in range(n_grp) if all(i == j for i, j in routes[k])]
    pieces = pl.pallas_call(
        functools.partial(pick_kernel, partners),
        out_shape=[jax.ShapeDtypeStruct((width, positions), jnp.bfloat16)] * n_grp,
        in_specs=[hbm],
        out_specs=whole(n_grp),
        scratch_shapes=[pltpu.SemaphoreType.DMA((n_grp,))],
        compiler_params=kernel_params(4),
        cost_estimate=pl.CostEstimate(flops=3 * 10**9, transcendentals=0, bytes_accessed=2 << 20),
        name="pick",
    )(in_hbm(by_width))
    caches = []
    for k, piece in enumerate(pieces):
        caches.append(piece if k in kept else lax.ppermute(piece, "grp", routes[k]))
    queries = pl.pallas_call(
        functools.partial(absorb_kernel, drafts, packed),
        out_shape=jax.ShapeDtypeStruct((n_seq,) + asked, jnp.bfloat16),
        in_specs=whole(3),
        out_specs=whole(1)[0],
        compiler_params=kernel_params(8),
        name="absorb",
    )(
        query_nope.reshape(requests, rows, nope),
        query_rope.reshape(requests, rows, rope),
        key_weight,
    )
    queries = lax.all_to_all(queries, "seq", 0, 0, tiled=True)

    partial = pl.pallas_call(
        functools.partial(attention_kernel, factor, latent, heads, drafts, partners, packed),
        out_shape=jax.ShapeDtypeStruct(
            (n_seq,) + given if packed else (n_seq * rows,) + given[1:], jnp.bfloat16
        ),
        in_specs=[smem] + whole(1 + n_grp),
        out_specs=whole(1)[0],
        compiler_params=kernel_params(12),
        cost_estimate=pl.CostEstimate(flops=6 * 10**9, transcendentals=0, bytes_accessed=3 << 20),
        name="attention",
    )(lengths, queries if packed else queries.reshape(n_seq * rows, width), *caches)

    received = lax.all_to_all(partial.reshape((n_seq,) + given), "seq", 0, 0, tiled=True)
    values = pl.pallas_call(
        functools.partial(merge_kernel, latent, packed),
        out_shape=jax.ShapeDtypeStruct((rows, value_weight.shape[2]), jnp.bfloat16),
        in_specs=whole(2),
        out_specs=whole(1)[0],
        scratch_shapes=[pltpu.VMEM((LANES, n_seq * STATS), jnp.float32)] * packed,
        compiler_params=kernel_params(8),
        name="merge",
    )(received, value_weight)
    values = lax.all_gather(values, "grp", axis=0, tiled=True)

    tokens = requests * drafts
    columns = output_weight.shape[1] // n_seq
    terms = pl.pallas_call(
        project_kernel,
        out_shape=jax.ShapeDtypeStruct((n_seq, tokens, columns), jnp.bfloat16),
        in_specs=whole(2),
        out_specs=whole(1)[0],
        scratch_shapes=[pltpu.VMEM(values.shape, jnp.float32)],
        compiler_params=kernel_params(12),
        name="project",
    )(values, output_weight)
    terms = lax.all_to_all(terms, "seq", 0, 0, tiled=True)
    mixed = jnp.sum(terms.astype(jnp.float32), axis=0).astype(jnp.bfloat16)
    return mixed.reshape(requests, drafts, columns)


def solution(mesh):
    in_specs = (
        P(None, None, "seq", None),
        P(None, None, "seq", None),
        P(None, ("seq", "grp"), None),
        P(),
        P("seq", None, None),
        P("seq", None, None),
        P("seq", "grp"),
    )
    out_specs = P(None, None, ("grp", "seq"))
    return jax.shard_map(shards, mesh=mesh, in_specs=in_specs, out_specs=out_specs, check_vma=False)
```

```python
import functools

import jax
import jax.numpy as jnp
from jax import lax
from jax.experimental import pallas as pl
from jax.experimental.pallas import tpu as pltpu
from jax.sharding import PartitionSpec as P


NEGATIVE = -1e30
LANES = 128
STATS = 8


def split3(x):
    high = x.astype(jnp.bfloat16).astype(jnp.float32)
    rest = x - high
    middle = rest.astype(jnp.bfloat16).astype(jnp.float32)
    return high, middle, rest - middle


def chunks(width):
    return range(width // LANES)


def packs(n_seq, drafts, heads, latent, rope):
    rows = drafts * heads
    return (
        heads % 16 == 0
        and latent % LANES == 0
        and drafts * rope == LANES
        and LANES % rows == 0
        and n_seq * rows % LANES == 0
        and n_seq <= LANES
    )


def unpack_queries(query, latent, heads, drafts):
    n_seq, _, lanes = query.shape
    rows = drafts * heads
    parts = [query[:, c * rows : (c + 1) * rows, :] for c in chunks(latent)]
    tail = query[:, len(parts) * rows :, :]
    owner = lax.broadcasted_iota(jnp.int32, tail.shape, 2) // (lanes // drafts)
    zero = jnp.zeros_like(tail)
    parts.append(
        jnp.concatenate([jnp.where(owner == t, tail, zero) for t in range(drafts)], axis=1)
    )
    parts = [part.reshape(n_seq * rows, lanes) for part in parts]
    return jnp.concatenate(parts[:-1], axis=-1), parts[-1]


def attention_kernel(factor, latent, heads, drafts, partners, packed, apart, lengths, *refs):
    if apart:
        query = refs[-1]
        seq = lax.axis_index("seq")
        for k in range(apart):
            query[seq ^ k] = refs[k][0]
        refs = refs[apart:-1]
    else:
        query, refs = refs[0], refs[1:]
    caches, out = refs[:-1], refs[-1]
    rows = query.shape[0] * drafts * heads if packed else query.shape[0]
    width = caches[0].shape[1]
    seq, grp = lax.axis_index("seq"), lax.axis_index("grp")
    token = (lax.broadcasted_iota(jnp.int32, (rows, 1), 0) // heads) % drafts
    limit = lengths[grp] - drafts + 1 + token
    queries = unpack_queries(query, latent, heads, drafts) if packed else query[...]
    scores = []
    for j, cache in enumerate(caches):
        if packed:
            tail = jnp.concatenate([cache[latent:, :]] * drafts, axis=0)
            raw = jnp.dot(queries[0], cache[:latent, :], preferred_element_type=jnp.float32)
            raw = raw + jnp.dot(queries[1], tail, preferred_element_type=jnp.float32)
        else:
            raw = jnp.dot(queries, cache[...], preferred_element_type=jnp.float32)
        raw = raw * factor
        offset = (seq * len(caches) + partners[j](grp)) * width
        places = offset + lax.broadcasted_iota(jnp.int32, (rows, width), 1)
        scores.append(jnp.where(places < limit, raw, NEGATIVE))
    top = functools.reduce(jnp.maximum, scores).max(axis=-1, keepdims=True)
    total = jnp.zeros((rows, 1), jnp.float32)
    summed = jnp.zeros((rows, latent), jnp.float32)
    for j, cache in enumerate(caches):
        expo = jnp.exp(scores[j] - top)
        total = total + jnp.sum(expo, axis=-1, keepdims=True)
        summed = summed + lax.dot_general(
            expo.astype(jnp.bfloat16),
            cache[:latent, :],
            (((1,), (1,)), ((), ())),
            preferred_element_type=jnp.float32,
        )
    result = (summed / total).astype(jnp.bfloat16)
    lane = lax.broadcasted_iota(jnp.int32, (rows, LANES), 1)
    if not packed:
        stats = jnp.zeros((rows, LANES), jnp.float32)
        for i, piece in enumerate(split3(top) + split3(total)):
            stats = jnp.where(lane == i, piece, stats)
        out[:, :latent] = result
        out[:, latent:] = stats.astype(jnp.bfloat16)
        return
    block = drafts * heads
    turned = jnp.where(lane == 0, top, total).T[:STATS]
    place = lax.broadcasted_iota(jnp.int32, (STATS, rows), 0)
    by_stat = jnp.zeros((STATS, rows), jnp.float32)
    for i, piece in enumerate(split3(turned[0:1]) + split3(turned[1:2])):
        by_stat = jnp.where(place == i, piece, by_stat)
    by_stat = by_stat.astype(jnp.bfloat16)
    for i in range(rows // block):
        for c in chunks(latent):
            lanes = slice(c * LANES, (c + 1) * LANES)
            out[i, c * block : (c + 1) * block, :] = result[i * block : (i + 1) * block, lanes]
        start = i * block // LANES * LANES
        out[i, len(chunks(latent)) * block :, :] = by_stat[:, start : start + LANES]


def stacked(array, heads):
    rows = array.shape[0]
    head = lax.broadcasted_iota(jnp.int32, (rows, 1), 0) % heads
    zero = jnp.zeros_like(array)
    return jnp.concatenate([jnp.where(head == h, array, zero) for h in range(heads)], axis=-1)


def pick_kernel(partners, cache, *refs):
    pieces, sems = refs[:-1], refs[-1]
    grp = lax.axis_index("grp")
    copies = [
        pltpu.make_async_copy(cache.at[partners[i](grp)], piece, sems.at[i])
        for i, piece in enumerate(pieces)
    ]
    for copy in copies:
        copy.start()
    for copy in copies:
        copy.wait()


def absorb_kernel(drafts, packed, nope, rope, weight, queries):
    grp = lax.axis_index("grp")
    heads, depth, latent = weight.shape
    absorbed = jnp.dot(
        stacked(nope[grp], heads),
        weight[...].reshape(heads * depth, latent),
        preferred_element_type=jnp.float32,
    ).astype(jnp.bfloat16)
    tail = rope[grp]
    if not packed:
        for i in range(queries.shape[0]):
            queries[i, :, :latent] = absorbed
            queries[i, :, latent:] = tail
        return
    parts = [absorbed[:, c * LANES : (c + 1) * LANES] for c in chunks(latent)]
    parts.append(
        jnp.concatenate([tail[t * heads : (t + 1) * heads] for t in range(drafts)], axis=-1)
    )
    block = jnp.concatenate(parts, axis=0)
    for i in range(queries.shape[0]):
        queries[i] = block


def merge_kernel(latent, packed, received, weight, out, *scratch):
    heads, depth, width = weight.shape
    rows = out.shape[0]
    sources = received.shape[0]
    if packed:
        turned = scratch[0]
        first = len(chunks(latent)) * rows
        stats = received[:, first:, :].astype(jnp.float32)
    else:
        block = received[...]
        stats = block[:, :, latent:].astype(jnp.float32)

    def stat(i):
        return stats[:, i, :] if packed else stats[:, :, i : i + 1]

    top = (stat(0) + stat(1)) + stat(2)
    shares = ((stat(3) + stat(4)) + stat(5)) * jnp.exp(top - jnp.max(top, axis=0, keepdims=True))
    shares = shares / jnp.sum(shares, axis=0, keepdims=True)
    if packed:
        turned[...] = jnp.concatenate([shares, jnp.zeros((LANES - sources, LANES), jnp.float32)]).T
        start = lax.axis_index("seq") * rows % LANES
        own = turned[pl.ds(pl.multiple_of(start, rows), rows), :]
        shares = [own[:, j : j + 1] for j in range(sources)]
        parts = [
            [received[j, c * rows : (c + 1) * rows, :] for j in range(sources)]
            for c in chunks(latent)
        ]
    else:
        parts = [[block[j, :, :latent] for j in range(sources)]]
    merged = jnp.concatenate(
        [
            functools.reduce(
                jnp.add, [shares[j] * piece.astype(jnp.float32) for j, piece in enumerate(part)]
            )
            for part in parts
        ],
        axis=-1,
    ).astype(jnp.bfloat16)
    values = jnp.dot(
        stacked(merged, heads),
        weight[...].reshape(heads * depth, width),
        preferred_element_type=jnp.float32,
    )
    out[...] = values.astype(jnp.bfloat16)


def project_kernel(values, weight, out, wide):
    tokens = out.shape[1]
    heads = values.shape[0] // tokens
    wide[...] = values[...].astype(jnp.float32)
    left = jnp.concatenate(
        [wide[pl.ds(h, tokens, stride=heads), :] for h in range(heads)], axis=-1
    ).astype(jnp.bfloat16)
    terms = jnp.dot(left, weight[...], preferred_element_type=jnp.float32)
    width = out.shape[2]
    for i in range(out.shape[0]):
        out[i] = terms[:, i * width : (i + 1) * width].astype(out.dtype)


def whole(count):
    return [pl.BlockSpec(memory_space=pltpu.VMEM)] * count


def in_hbm(array):
    return pltpu.with_memory_space_constraint(array, pltpu.HBM)


def kernel_params(mebibytes):
    return pltpu.CompilerParams(vmem_limit_bytes=mebibytes << 20)


def shards(query_nope, query_rope, latent_cache, lengths, key_weight, value_weight, output_weight):
    n_seq, n_grp = lax.axis_size("seq"), lax.axis_size("grp")
    requests, drafts, heads, nope = query_nope.shape
    rope = query_rope.shape[3]
    latent = key_weight.shape[2]
    positions, width = latent_cache.shape[1:]
    factor = float(nope + rope) ** (-0.5)
    rows = drafts * heads
    assert requests == n_grp
    packed = packs(n_seq, drafts, heads, latent, rope)
    apart = n_seq if packed and n_seq in (2, 4, 8) else 0
    asked = (rows * len(chunks(latent)) + heads, LANES) if packed else (rows, width)
    given = (rows * len(chunks(latent)) + STATS, LANES) if packed else (rows, latent + LANES)

    def partner(k):
        if n_grp & (n_grp - 1) == 0:
            return lambda i: i ^ k
        return lambda i: (k - i) % n_grp

    partners = [partner(k) for k in range(n_grp)]
    by_width = jnp.swapaxes(latent_cache, 1, 2)
    smem = pl.BlockSpec(memory_space=pltpu.SMEM)
    hbm = pl.BlockSpec(memory_space=pltpu.HBM)
    routes = [[(i, other(i)) for i in range(n_grp)] for other in partners]
    kept = [k for k in range(n_grp) if all(i == j for i, j in routes[k])]
    pieces = pl.pallas_call(
        functools.partial(pick_kernel, partners),
        out_shape=[jax.ShapeDtypeStruct((width, positions), jnp.bfloat16)] * n_grp,
        in_specs=[hbm],
        out_specs=whole(n_grp),
        scratch_shapes=[pltpu.SemaphoreType.DMA((n_grp,))],
        compiler_params=kernel_params(4),
        cost_estimate=pl.CostEstimate(flops=3 * 10**9, transcendentals=0, bytes_accessed=2 << 20),
        name="pick",
    )(in_hbm(by_width))
    caches = []
    for k, piece in enumerate(pieces):
        caches.append(piece if k in kept else lax.ppermute(piece, "grp", routes[k]))
    queries = pl.pallas_call(
        functools.partial(absorb_kernel, drafts, packed),
        out_shape=jax.ShapeDtypeStruct((1 if apart else n_seq,) + asked, jnp.bfloat16),
        in_specs=whole(3),
        out_specs=whole(1)[0],
        compiler_params=kernel_params(8),
        name="absorb",
    )(
        query_nope.reshape(requests, rows, nope),
        query_rope.reshape(requests, rows, rope),
        key_weight,
    )
    if apart:
        arrived = {0: queries}
        for k in range(1, n_seq):
            arrived[k] = lax.ppermute(queries, "seq", [(i, i ^ k) for i in range(n_seq)])
        queries = [arrived[k] for k in range(n_seq)]
    else:
        queries = lax.all_to_all(queries, "seq", 0, 0, tiled=True)
        queries = [queries if packed else queries.reshape(n_seq * rows, width)]

    partial = pl.pallas_call(
        functools.partial(attention_kernel, factor, latent, heads, drafts, partners, packed, apart),
        out_shape=jax.ShapeDtypeStruct(
            (n_seq,) + given if packed else (n_seq * rows,) + given[1:], jnp.bfloat16
        ),
        in_specs=[smem] + whole(len(queries) + n_grp),
        out_specs=whole(1)[0],
        scratch_shapes=[pltpu.VMEM((n_seq,) + asked, jnp.bfloat16)] if apart else [],
        compiler_params=kernel_params(12),
        cost_estimate=pl.CostEstimate(flops=6 * 10**9, transcendentals=0, bytes_accessed=3 << 20),
        name="attention",
    )(lengths, *queries, *caches)

    received = lax.all_to_all(partial.reshape((n_seq,) + given), "seq", 0, 0, tiled=True)
    values = pl.pallas_call(
        functools.partial(merge_kernel, latent, packed),
        out_shape=jax.ShapeDtypeStruct((rows, value_weight.shape[2]), jnp.bfloat16),
        in_specs=whole(2),
        out_specs=whole(1)[0],
        scratch_shapes=[pltpu.VMEM((LANES, LANES), jnp.float32)] * packed,
        compiler_params=kernel_params(8),
        name="merge",
    )(received, value_weight)
    values = lax.all_gather(values, "grp", axis=0, tiled=True)

    tokens = requests * drafts
    columns = output_weight.shape[1] // n_seq
    terms = pl.pallas_call(
        project_kernel,
        out_shape=jax.ShapeDtypeStruct((n_seq, tokens, columns), jnp.bfloat16),
        in_specs=whole(2),
        out_specs=whole(1)[0],
        scratch_shapes=[pltpu.VMEM(values.shape, jnp.float32)],
        compiler_params=kernel_params(12),
        name="project",
    )(values, output_weight)
    terms = lax.all_to_all(terms, "seq", 0, 0, tiled=True)
    mixed = jnp.sum(terms.astype(jnp.float32), axis=0).astype(jnp.bfloat16)
    return mixed.reshape(requests, drafts, columns)


def solution(mesh):
    in_specs = (
        P(None, None, "seq", None),
        P(None, None, "seq", None),
        P(None, ("seq", "grp"), None),
        P(),
        P("seq", None, None),
        P("seq", None, None),
        P("seq", "grp"),
    )
    out_specs = P(None, None, ("grp", "seq"))
    return jax.shard_map(shards, mesh=mesh, in_specs=in_specs, out_specs=out_specs, check_vma=False)
```
